32 devices in a mesh: dp: 4 (over y, x), expert: 8 (over z, core).
Axes of the slice: x: 2, y: 2, z: 4, core: 2. Of those that a mesh axis runs over, the one named last changes fastest.
Arguments:
- tokens: bfloat16 [4096, 2048], P(('dp', 'expert')), may hold values from -6 to 6
- expert_ids: int32 [4096, 2], P(('dp', 'expert')), may hold values from 0 to 7, all different within a row; in each aligned block of 128 rows (0 to 127, 128 to 255, ...) at most 40 rows name the same one
- gate_units: int32 [4096, 2], P(('dp', 'expert')), may hold values from 64 to 1023
- capacity: int32 [8], replicated, may hold values from 512 to 1535
- w_gate: bfloat16 [8, 2048, 1408], P('expert', None, 'dp'), may hold values from -0.125 to 0.125
- w_up: bfloat16 [8, 2048, 1408], P('expert', None, 'dp'), may hold values from -0.125 to 0.125
- w_down: bfloat16 [8, 2048, 1408], P('expert', None, 'dp'), may hold values from -0.15625 to 0.15625
Outputs:
- mixed: bfloat16 [4096, 2048], P(('dp', 'expert'))
The draws below stay inside these ranges and needn't reach their ends.
Inputs may be any that keep to these rules, and one draw needn't show every extreme that they name: `expert_ids`: each row names two different experts; of one device's 128 rows (aligned blocks) no expert is named more than 40 times.
All inputs are finite; a program needn't handle non-finite values.
Results may differ from the reference program's by a relative error of at most 0.0057.
Values may be sent and summed in bfloat16 or wider, within the bound.
A program may use at most 128 MiB of HBM per device.

```python
import math
import jax
import jax.numpy as jnp
import numpy as np
from jax import lax

D = 2048
FF = 1408
TOK_DEV = 128
EXPERTS = 8
TOKENS = 4096
MOST = 40
CAP_HI = 1536


def touch_ends(values, key, low, top_value):
    place = [jax.random.randint(jax.random.fold_in(key, axis), (), 0, length) for axis, length in enumerate(values.shape)]
    main_axis = values.shape.index(max(values.shape))
    neighbour = place[:main_axis] + [(place[main_axis] + 1) % values.shape[main_axis]] + place[main_axis + 1:]
    return values.at[tuple(place)].set(low).at[tuple(neighbour)].set(top_value)


def level_of(key, shape, split, smallest, top_value):
    loudness, own = 1.0, jax.random.fold_in(key, 6)
    for position, shards_of in split:
        heights = jnp.exp(jax.random.uniform(jax.random.fold_in(own, position), (shards_of,), jnp.float32, smallest / len(split), top_value / len(split)))
        loudness = loudness * jnp.repeat(heights, shape[position] // shards_of).reshape([-1 if axis == position else 1 for axis in range(len(shape))])
    return loudness


def routed_block(key, own, number, rows, number_of, top, limit, lean):
    sequence = jax.random.permutation(key, number_of)
    packed, ordinary = load_shares(number_of, rows * top, limit, lean, True), load_shares(number_of, rows * top, limit, lean, False)
    places = jnp.arange(number_of)

    def named(lengths, turn):
        used = int((lengths > 0).sum())
        fixed = max(1, used // 4)
        shifted = fixed + (places - fixed + turn * (used - fixed)) % max(1, number_of - fixed)
        return jnp.zeros((number_of,), jnp.int32).at[sequence[jnp.where(places < fixed, places, shifted)]].set(jnp.asarray(lengths, jnp.int32))

    lengths = jnp.where(number % 4 == 0, named(packed, number // 4), named(ordinary, number - number // 4 - 1))
    mixed = jax.random.permutation(jax.random.fold_in(own, 3), number_of)
    giver, taker = mixed[0:number_of // 2 * 2:2], mixed[1:number_of // 2 * 2:2]
    room = jnp.minimum(lengths[giver] - 1, limit - lengths[taker]) // 2
    room = jnp.where((giver == sequence[0]) | (taker == sequence[0]) | (lengths[taker] == 0), 0, jnp.maximum(room, 0))
    shifted = jax.random.randint(jax.random.fold_in(own, 4), (number_of // 2,), 0, 1 << 20) % (room + 1)
    lengths = lengths.at[giver].add(-shifted).at[taker].add(shifted)
    items = jnp.searchsorted(jnp.cumsum(lengths), jnp.arange(rows * top), side="right").astype(jnp.int32)
    listing = items.reshape(top, rows).T
    listing = listing[jax.random.permutation(jax.random.fold_in(own, 1), rows)]
    turn = jax.random.randint(jax.random.fold_in(own, 2), (rows, 1), 0, top)
    return jnp.take_along_axis(listing, (jnp.arange(top)[None, :] + turn) % top, axis=1)


def load_shares(amount, total, limit, skew, full):
    weights = [(1 << 20) // math.isqrt(standing ** skew) + 1 for standing in range(1, amount + 1)]
    largest = limit if full else min(limit, max(-(-total // amount), total * weights[0] // sum(weights)))
    least = 1 if total - largest >= amount - 1 else 0
    counts, spare = [largest] + [least] * (amount - 1), total - largest - least * (amount - 1)
    while spare > 0:
        movable = [i for i in range(1, amount) if counts[i] < largest] or [i for i in range(1, amount) if counts[i] < limit]
        whole, left = sum([weights[i] for i in movable]), spare
        for i in movable:
            extra = min(limit - counts[i], max(1, left * weights[i] // whole), spare)
            counts[i] = counts[i] + extra
            spare = spare - extra
    return np.array(counts)


def noise(key, dims, width, limit, shards=(), kind=jnp.bfloat16):
    loudness = level_of(key, dims, shards, -0.22, 0.18) if shards else 1.0
    values = jax.random.normal(key, dims, jnp.float32) * width * loudness
    return jnp.minimum(jnp.maximum(values, -limit), limit).astype(kind)


def setup_inputs(seed: int = 0) -> dict:
    arg_keys = jax.random.split(jax.random.key(seed), 8)
    tokens = noise(arg_keys[0], (TOKENS, D), 1.0, 6.0, ((0, 32),))
    expert_ids_keys = jax.random.split(jax.random.fold_in(arg_keys[1], 1), TOKENS // TOK_DEV)
    expert_ids_turns = jax.random.permutation(jax.random.fold_in(arg_keys[1], 3), TOKENS // TOK_DEV)
    expert_ids = jax.vmap(lambda own, number: routed_block(jax.random.fold_in(arg_keys[1], 2), own, number, TOK_DEV, EXPERTS, 2, MOST, 1))(expert_ids_keys, expert_ids_turns).reshape((TOKENS, 2))
    gate_units = touch_ends(jax.random.randint(arg_keys[2], (TOKENS, 2), 64, 1024), jax.random.fold_in(arg_keys[2], 1), 64, 1023).astype(jnp.int32)
    capacity = touch_ends(jax.random.randint(arg_keys[3], (EXPERTS,), TOKENS // EXPERTS, CAP_HI), jax.random.fold_in(arg_keys[3], 1), TOKENS // EXPERTS, CAP_HI - 1).astype(jnp.int32)
    w_gate = noise(arg_keys[4], (EXPERTS, D, FF), D ** -0.5, 0.125, ((0, 8), (2, 4)))
    w_up = noise(arg_keys[5], (EXPERTS, D, FF), D ** -0.5, 0.125, ((0, 8), (2, 4)))
    w_down = noise(arg_keys[6], (EXPERTS, D, FF), FF ** -0.5, 0.15625, ((0, 8), (2, 4)))
    return {"tokens": tokens, "expert_ids": expert_ids, "gate_units": gate_units, "capacity": capacity, "w_gate": w_gate, "w_up": w_up, "w_down": w_down}


def expert_rows(rows, gate_w, up_w, down_w):
    gate = jnp.dot(rows, gate_w, preferred_element_type=jnp.float32)
    up = jnp.dot(rows, up_w, preferred_element_type=jnp.float32)
    hidden = (jax.nn.silu(gate) * up).astype(jnp.bfloat16)
    return lax.dot_general(hidden, down_w, (((1,), (1,)), ((), ())), preferred_element_type=jnp.float32)


def reference(tokens, expert_ids, gate_units, capacity, w_gate, w_up, w_down):
    flat = expert_ids.reshape(-1).astype(jnp.int32)
    onehot = (flat[:, None] == jnp.arange(EXPERTS, dtype=jnp.int32)[None, :]).astype(jnp.int32)
    slot = jnp.sum((jnp.cumsum(onehot, axis=0) - onehot) * onehot, axis=1).astype(jnp.int32)
    kept = slot < capacity[flat]
    weight = jnp.where(kept, gate_units.reshape(-1).astype(jnp.float32) / 1024.0, jnp.float32(0.0))
    token_of = (jnp.arange(2 * TOKENS, dtype=jnp.int32) // 2).astype(jnp.int32)

    def per_expert(carry, index):
        target = jnp.where((flat == index) & kept, slot, CAP_HI).astype(jnp.int32)
        rows_index = jnp.zeros((CAP_HI,), jnp.int32).at[target].set(token_of, mode="drop")
        scales = jnp.zeros((CAP_HI,), jnp.float32).at[target].set(weight, mode="drop")
        result = expert_rows(tokens[rows_index], w_gate[index], w_up[index], w_down[index])
        result = result.astype(jnp.bfloat16).astype(jnp.float32)
        carry = carry.at[rows_index].add(result * scales[:, None])
        return carry, None

    total, _ = lax.scan(per_expert, jnp.zeros((TOKENS, D), jnp.float32), jnp.arange(EXPERTS, dtype=jnp.int32))
    return total.astype(jnp.bfloat16)
```

```python
import functools

import jax
import jax.numpy as jnp
from jax import lax
from jax.experimental import pallas as pl
from jax.experimental.pallas import tpu as pltpu
from jax.sharding import PartitionSpec as P

MESH = pl.DeviceIdType.MESH


def exchange(
    n, out_ref, wg_ref, wu_ref, wd_ref, back_ref,
    xin, part, got1, sums, got2, ans,
    zs, zr, as_, ar, bs, br, cs, cr, ds, dr, es, er, loc,
):
    d = lax.axis_index("dp")
    e = lax.axis_index("expert")
    across = d + 1 - 2 * lax.rem(d, 2)
    along = lax.rem(d + 2, 4)
    most, half = xin.shape[3], xin.shape[4]
    near = ((across, e), (along, e))

    def remote(src, dst, send, recv, device):
        return pltpu.make_async_remote_copy(
            src_ref=src, dst_ref=dst, send_sem=send, recv_sem=recv,
            device_id=device, device_id_type=MESH,
        )

    def ahead(k):
        return (d, lax.rem(e + k, n))

    def behind(k):
        return (d, lax.rem(e + n - k, n))

    def to_owner(k):
        target = ahead(k)
        return remote(out_ref.at[target[1]], xin.at[k, 0], zs.at[k], zr.at[k], target)

    def spread(i, r):
        return remote(xin.at[i, 0], xin.at[i, 1 + r], as_.at[i, r], ar.at[i, r], near[r])

    def relay(i, r):
        return remote(
            xin.at[i, 1 + r, r], xin.at[i, 3, r], bs.at[i, r], br.at[i, r], near[1 - r]
        )

    def first(i, r):
        return remote(
            part.at[i, r, pl.ds(0, 2)], got1.at[i, r], cs.at[i, r], cr.at[i, r], near[r]
        )

    def second(i, r):
        return remote(sums.at[i, r], got2.at[i, r], ds.at[i, r], dr.at[i, r], near[1 - r])

    def give_back(i):
        return remote(ans.at[i], back_ref.at[e], es.at[i], er.at[i], behind(i))

    barrier = pltpu.get_barrier_semaphore()

    def greet(k, carry):
        pl.semaphore_signal(barrier, inc=1, device_id=ahead(k), device_id_type=MESH)
        return carry

    lax.fori_loop(1, n, greet, 0)
    for r in range(2):
        pl.semaphore_signal(barrier, inc=1, device_id=near[r], device_id_type=MESH)
    pl.semaphore_wait(barrier, n + 1)

    def launch(k, carry):
        to_owner(k).start()
        return carry

    own = pltpu.make_async_copy(out_ref.at[e], xin.at[0, 0], loc.at[0])
    own.start()
    lax.fori_loop(1, n, launch, 0)
    own.wait()

    def stage_a(i):
        @pl.when(i > 0)
        def _():
            to_owner(i).wait_recv()

        for r in range(2):
            spread(i, r).start()

    def stage_b(i):
        for r in range(2):
            spread(i, r).wait_recv()
            relay(i, r).start()

    def stage_c(i):
        for r in range(2):
            relay(i, r).wait_recv()
        gate = up = None
        for h in range(2):
            rows = xin[i, :, h].reshape(4 * most, half)
            g = jnp.dot(rows, wg_ref[0, pl.ds(h * half, half), :], preferred_element_type=jnp.float32)
            u = jnp.dot(rows, wu_ref[0, pl.ds(h * half, half), :], preferred_element_type=jnp.float32)
            gate, up = (g, u) if h == 0 else (gate + g, up + u)
        hidden = (gate / (1.0 + jnp.exp(-gate)) * up).astype(jnp.bfloat16)
        for h in range(2):
            made = lax.dot_general(
                hidden, wd_ref[0, pl.ds(h * half, half), :], (((1,), (1,)), ((), ())),
                preferred_element_type=jnp.float32,
            )
            for slot, block in enumerate(((1, 3, 0, 2), (2, 3, 0, 1))[h]):
                part[i, h, slot] = made[block * most:(block + 1) * most].astype(jnp.bfloat16)
            first(i, h).start()

    def stage_d(i):
        for r in range(2):
            first(i, r).wait_recv()
            total = part[i, r, 3].astype(jnp.float32) + got1[i, r, 1].astype(jnp.float32)
            sums[i, r] = total.astype(jnp.bfloat16)
            second(i, r).start()

    def stage_e(i):
        for r in range(2):
            second(i, r).wait_recv()
            total = (
                part[i, r, 2].astype(jnp.float32)
                + got1[i, r, 0].astype(jnp.float32)
                + got2[i, r].astype(jnp.float32)
            )
            ans[i, r] = total.astype(jnp.bfloat16)

        @pl.when(i > 0)
        def _():
            give_back(i).start()

        @pl.when(i == 0)
        def _():
            kept_here = pltpu.make_async_copy(ans.at[0], back_ref.at[e], loc.at[0])
            kept_here.start()
            kept_here.wait()

    stages = (stage_a, stage_b, stage_c, stage_d, stage_e)

    def step(t, carry):
        for lag, stage in reversed(list(enumerate(stages))):
            @pl.when((t >= lag) & (t < n + lag))
            def _(stage=stage, lag=lag):
                stage(t - lag)
        return carry

    lax.fori_loop(0, n + len(stages) - 1, step, 0)

    def settle(i, carry):
        for r in range(2):
            spread(i, r).wait_send()
            relay(i, r).wait_send()
            first(i, r).wait_send()
            second(i, r).wait_send()

        @pl.when(i > 0)
        def _():
            to_owner(i).wait_send()
            give_back(i).wait()

        return carry

    lax.fori_loop(0, n, settle, 0)


def experts(outgoing, w_gate, w_up, w_down):
    n, _, most, half = outgoing.shape
    bf16 = jnp.bfloat16
    vmem = pl.BlockSpec(memory_space=pltpu.VMEM)
    dma = pltpu.SemaphoreType.DMA
    return pl.pallas_call(
        functools.partial(exchange, n),
        out_shape=jax.ShapeDtypeStruct(outgoing.shape, bf16),
        in_specs=[vmem] * 4,
        out_specs=vmem,
        scratch_shapes=[
            pltpu.VMEM((n, 4, 2, most, half), bf16),
            pltpu.VMEM((n, 2, 4, most, half), bf16),
            pltpu.VMEM((n, 2, 2, most, half), bf16),
            pltpu.VMEM((n, 2, most, half), bf16),
            pltpu.VMEM((n, 2, most, half), bf16),
            pltpu.VMEM((n, 2, most, half), bf16),
            dma((n,)), dma((n,)),
            dma((n, 2)), dma((n, 2)),
            dma((n, 2)), dma((n, 2)),
            dma((n, 2)), dma((n, 2)),
            dma((n, 2)), dma((n, 2)),
            dma((n,)), dma((n,)),
            dma((1,)),
        ],
        compiler_params=pltpu.CompilerParams(
            collective_id=0, has_side_effects=True, vmem_limit_bytes=60 * 1024 * 1024
        ),
    )(outgoing, w_gate, w_up, w_down)


def local(tokens, expert_ids, gate_units, capacity, w_gate, w_up, w_down):
    tok_rows, width = tokens.shape
    n_experts = capacity.shape[0]
    most = max(2, 5 * tok_rows // (2 * n_experts))
    most = -(-most // 8) * 8
    slots_all = n_experts * most
    half = width // 2
    flat = expert_ids.reshape(-1)
    onehot = (flat[:, None] == jnp.arange(n_experts, dtype=jnp.int32)[None, :]).astype(jnp.int32)
    local_rank = jnp.sum((jnp.cumsum(onehot, axis=0) - onehot) * onehot, axis=1)
    send_slot = flat * most + local_rank
    chosen = send_slot.reshape(tok_rows, 2)[:, :, None] == jnp.arange(slots_all, dtype=jnp.int32)
    placing = (chosen[:, 0] | chosen[:, 1]).astype(jnp.bfloat16)
    outgoing = jnp.stack(
        [
            lax.dot_general(
                placing, tokens[:, h * half:(h + 1) * half], (((0,), (0,)), ((), ())),
                preferred_element_type=jnp.float32,
            ).astype(jnp.bfloat16).reshape(n_experts, most, half)
            for h in range(2)
        ],
        axis=1,
    )
    back = experts(outgoing, w_gate, w_up, w_down)

    counts = jnp.sum(onehot, axis=0)
    everything = lax.all_gather(counts, ("dp", "expert"))
    here = lax.axis_index(("dp", "expert"))
    earlier = jnp.arange(everything.shape[0], dtype=jnp.int32)[:, None] < here
    offsets = jnp.sum(jnp.where(earlier, everything, 0), axis=0)
    room = jnp.sum(onehot * (capacity - offsets)[None, :], axis=1)
    kept = local_rank < room
    units = jnp.where(kept, gate_units.reshape(-1), 0).reshape(tok_rows, 2)
    placed = jnp.sum(jnp.where(chosen, units[:, :, None], 0), axis=1)
    low = placed % 8
    high = (placed - low).astype(jnp.bfloat16)
    low = low.astype(jnp.bfloat16)
    mixed = []
    for h in range(2):
        rows = back[:, h].reshape(slots_all, half)
        total = jnp.dot(high, rows, preferred_element_type=jnp.float32) + jnp.dot(
            low, rows, preferred_element_type=jnp.float32
        )
        mixed.append((total * (1.0 / 1024.0)).astype(jnp.bfloat16))
    return jnp.concatenate(mixed, axis=1)


def solution(mesh):
    return jax.shard_map(
        local,
        mesh=mesh,
        in_specs=(
            P(("dp", "expert"), None),
            P(("dp", "expert"), None),
            P(("dp", "expert"), None),
            P(),
            P("expert", None, "dp"),
            P("expert", None, "dp"),
            P("expert", None, "dp"),
        ),
        out_specs=P(("dp", "expert"), None),
        check_vma=False,
    )
```

```python
import functools

import jax
import jax.numpy as jnp
from jax import lax
from jax.experimental import pallas as pl
from jax.experimental.pallas import tpu as pltpu
from jax.sharding import PartitionSpec as P

MESH = pl.DeviceIdType.MESH


def exchange(
    n, most, tok_ref, ids_ref, turned_ref, units_ref, cap_ref, wg_hbm, wu_hbm, wd_hbm, out_ref,
    wg_ref, wu_ref, wd_ref, outgoing, xin, part, got1, sums, got2, ans, back, acc, code, scale, table,
    zs, zr, as_, ar, bs, br, cs, cr, ds, dr, es, er, ks, kr, ts, tr, loc,
):
    d = lax.axis_index("dp")
    e = lax.axis_index("expert")
    across = d + 1 - 2 * lax.rem(d, 2)
    along = lax.rem(d + 2, 4)
    diagonal = lax.rem(across + 2, 4)
    half = xin.shape[4]
    tok_rows = tok_ref.shape[0]
    lanes = table.shape[3]
    near = ((across, e), (along, e))
    f32, bf16 = jnp.float32, jnp.bfloat16

    def remote(src, dst, send, recv, device):
        return pltpu.make_async_remote_copy(
            src_ref=src, dst_ref=dst, send_sem=send, recv_sem=recv,
            device_id=device, device_id_type=MESH,
        )

    def ahead(k):
        return (d, lax.rem(e + k, n))

    def behind(k):
        return (d, lax.rem(e + n - k, n))

    def to_owner(k):
        return remote(outgoing.at[k], xin.at[k, 0], zs.at[k], zr.at[k], ahead(k))

    def spread(i, r):
        return remote(xin.at[i, 0], xin.at[i, 1 + r], as_.at[i, r], ar.at[i, r], near[r])

    def relay(i, r):
        return remote(
            xin.at[i, 1 + r, r], xin.at[i, 3, r], bs.at[i, r], br.at[i, r], near[1 - r]
        )

    def first(i, r):
        return remote(
            part.at[i, r, pl.ds(0, 2)], got1.at[i, r], cs.at[i, r], cr.at[i, r], near[r]
        )

    def second(i, r):
        return remote(sums.at[i, r], got2.at[i, r], ds.at[i, r], dr.at[i, r], near[1 - r])

    def give_back(i):
        return remote(ans.at[i], back.at[i], es.at[i], er.at[i], behind(i))

    def count_out(k):
        return remote(table.at[0, 0], table.at[0, k], ks.at[k], kr.at[k], ahead(k))

    def table_near(r):
        return remote(table.at[0], table.at[1 + r], ts.at[r], tr.at[r], near[r])

    def table_far():
        return remote(table.at[1], table.at[3], ts.at[2], tr.at[2], near[1])

    def weights():
        return [
            pltpu.make_async_copy(hbm.at[0], vmem, loc.at[1 + w])
            for w, (hbm, vmem) in enumerate(((wg_hbm, wg_ref), (wu_hbm, wu_ref), (wd_hbm, wd_ref)))
        ]

    barrier = pltpu.get_barrier_semaphore()

    def greet(k, carry):
        pl.semaphore_signal(barrier, inc=1, device_id=ahead(k), device_id_type=MESH)
        return carry

    lax.fori_loop(1, n, greet, 0)
    for r in range(2):
        pl.semaphore_signal(barrier, inc=1, device_id=near[r], device_id_type=MESH)
    for copy in weights():
        copy.start()

    def iota(shape, axis):
        return lax.broadcasted_iota(jnp.int32, shape, axis)

    square = (tok_rows, tok_rows)
    ids = ids_ref[...]
    hot = [(iota((tok_rows, lanes), 1) == ids[:, k:k + 1]) for k in range(2)]
    named = jnp.where(hot[0] | hot[1], 1.0, 0.0)
    table[0, 0] = jnp.sum(named, axis=0, keepdims=True).astype(jnp.int32)
    lower = jnp.where(iota(square, 1) < iota(square, 0), 1.0, 0.0).astype(bf16)
    before = jnp.dot(lower, named.astype(bf16), preferred_element_type=f32)
    rank = [jnp.sum(jnp.where(h, before, 0.0), axis=1, keepdims=True) for h in hot]
    for k in range(2):
        slot = ids[:, k:k + 1] * most + rank[k].astype(jnp.int32)
        code[k] = jnp.broadcast_to(slot, (tok_rows, most))

    turned = turned_ref[...]
    hot_t = [(iota((n, tok_rows), 0) == turned[k:k + 1, :]) for k in range(2)]
    named_t = jnp.where(hot_t[0] | hot_t[1], 1.0, 0.0).astype(bf16)
    upper = jnp.where(iota(square, 0) < iota(square, 1), 1.0, 0.0).astype(bf16)
    before_t = jnp.dot(named_t, upper, preferred_element_type=f32)
    code_t = [
        turned[k:k + 1, :] * most
        + jnp.sum(jnp.where(hot_t[k], before_t, 0.0), axis=0, keepdims=True).astype(jnp.int32)
        for k in range(2)
    ]

    def rows_for(p, h):
        wanted = iota((most, tok_rows), 0) + p * most
        placing = jnp.where((code_t[0] == wanted) | (code_t[1] == wanted), 1.0, 0.0).astype(bf16)
        return jnp.dot(
            placing, tok_ref[:, h * half:(h + 1) * half], preferred_element_type=f32
        ).astype(bf16)

    for h in range(2):
        xin[0, 0, h] = rows_for(e, h)

    pl.semaphore_wait(barrier, n + 1)

    def counted(k, carry):
        count_out(k).start()
        return carry

    def launch(k, carry):
        for h in range(2):
            outgoing[k, h] = rows_for(ahead(k)[1], h)
        to_owner(k).start()
        return carry

    for r in range(2):
        spread(0, r).start()
    lax.fori_loop(1, n, counted, 0)
    lax.fori_loop(1, n, launch, 0)
    acc[...] = jnp.zeros_like(acc)

    def stage_a(i):
        @pl.when(i > 0)
        def _():
            to_owner(i).wait_recv()
            for r in range(2):
                spread(i, r).start()

    def stage_b(i):
        for r in range(2):
            spread(i, r).wait_recv()
            relay(i, r).start()

    def stage_c(i):
        @pl.when(i == 0)
        def _():
            for copy in weights():
                copy.wait()

        for r in range(2):
            relay(i, r).wait_recv()
        gate = up = None
        for h in range(2):
            rows = xin[i, :, h].reshape(4 * most, half)
            g = jnp.dot(rows, wg_ref[pl.ds(h * half, half), :], preferred_element_type=f32)
            u = jnp.dot(rows, wu_ref[pl.ds(h * half, half), :], preferred_element_type=f32)
            gate, up = (g, u) if h == 0 else (gate + g, up + u)
        hidden = (gate / (1.0 + jnp.exp(-gate)) * up).astype(bf16)
        for h in range(2):
            made = lax.dot_general(
                hidden, wd_ref[pl.ds(h * half, half), :], (((1,), (1,)), ((), ())),
                preferred_element_type=f32,
            )
            for slot, block in enumerate(((1, 3, 0, 2), (2, 3, 0, 1))[h]):
                part[i, h, slot] = made[block * most:(block + 1) * most].astype(bf16)
            first(i, h).start()

    def stage_d(i):
        for r in range(2):
            first(i, r).wait_recv()
            total = part[i, r, 3].astype(f32) + got1[i, r, 1].astype(f32)
            sums[i, r] = total.astype(bf16)
            second(i, r).start()

    def stage_e(i):
        for r in range(2):
            second(i, r).wait_recv()
            total = (
                part[i, r, 2].astype(f32) + got1[i, r, 0].astype(f32) + got2[i, r].astype(f32)
            )
            ans[i, r] = total.astype(bf16)

        @pl.when(i > 0)
        def _():
            give_back(i).start()

        @pl.when(i == 0)
        def _():
            kept_here = pltpu.make_async_copy(ans.at[0], back.at[0], loc.at[0])
            kept_here.start()
            kept_here.wait()

    def stage_f(i):
        @pl.when(i > 0)
        def _():
            give_back(i).wait_recv()

        wanted = iota((tok_rows, most), 1) + ahead(i)[1] * most
        placed = jnp.where(code[0] == wanted, scale[0], 0) + jnp.where(code[1] == wanted, scale[1], 0)
        low = placed & 7
        high = (placed - low).astype(f32).astype(bf16)
        low = low.astype(f32).astype(bf16)
        for h in range(2):
            rows = back[i, h]
            acc[:, h * half:(h + 1) * half] += jnp.dot(
                high, rows, preferred_element_type=f32
            ) + jnp.dot(low, rows, preferred_element_type=f32)

    def counts_near():
        def arrived(k, carry):
            count_out(k).wait_recv()
            return carry

        lax.fori_loop(1, n, arrived, 0)
        for r in range(2):
            table_near(r).start()

    def counts_far():
        for r in range(2):
            table_near(r).wait_recv()
        table_far().start()

    def counts_used():
        table_far().wait_recv()
        here = d * n + e
        offsets = jnp.zeros((1, lanes), jnp.int32)
        for s, row in enumerate((d, across, along, diagonal)):
            def add(k, total, s=s, row=row):
                earlier = row * n + behind(k)[1] < here
                return total + table[s, k] * earlier.astype(jnp.int32)

            offsets = lax.fori_loop(0, n, add, offsets)
        room = (cap_ref[...] - offsets).astype(f32)
        for k in range(2):
            limit = jnp.sum(jnp.where(hot[k], room, 0.0), axis=1, keepdims=True)
            units = jnp.where(rank[k] < limit, units_ref[:, k:k + 1], 0)
            scale[k] = jnp.broadcast_to(units, (tok_rows, most))

    stages = ((0, stage_a), (2, stage_b), (4, stage_c), (6, stage_d), (8, stage_e), (10, stage_f))

    def step(t, carry):
        for lag, stage in stages:
            @pl.when((t >= lag) & (t < n + lag))
            def _(stage=stage, lag=lag):
                stage(t - lag)
        for when, chore in ((3, counts_near), (5, counts_far), (7, counts_used)):
            pl.when(t == when)(chore)
        return carry

    lax.fori_loop(0, n + stages[-1][0], step, 0)
    out_ref[...] = (acc[...] * (1.0 / 1024.0)).astype(out_ref.dtype)

    def settle(i, carry):
        for r in range(2):
            spread(i, r).wait_send()
            relay(i, r).wait_send()
            first(i, r).wait_send()
            second(i, r).wait_send()

        @pl.when(i > 0)
        def _():
            to_owner(i).wait_send()
            give_back(i).wait_send()
            count_out(i).wait_send()

        return carry

    lax.fori_loop(0, n, settle, 0)
    for r in range(2):
        table_near(r).wait_send()
    table_far().wait_send()


def local(tokens, expert_ids, gate_units, capacity, w_gate, w_up, w_down):
    tok_rows, width = tokens.shape
    n = capacity.shape[0]
    most = max(2, 5 * tok_rows // (2 * n))
    most = -(-most // 8) * 8
    half = width // 2
    lanes = -(-n // 128) * 128
    bf16 = jnp.bfloat16
    vmem = pl.BlockSpec(memory_space=pltpu.VMEM)
    hbm = pl.BlockSpec(memory_space=pl.ANY)
    dma = pltpu.SemaphoreType.DMA
    block = (most, half)
    return pl.pallas_call(
        functools.partial(exchange, n, most),
        out_shape=jax.ShapeDtypeStruct(tokens.shape, bf16),
        in_specs=[vmem] * 5 + [hbm] * 3,
        out_specs=vmem,
        scratch_shapes=[
            pltpu.VMEM(w_gate.shape[1:], bf16),
            pltpu.VMEM(w_up.shape[1:], bf16),
            pltpu.VMEM(w_down.shape[1:], bf16),
            pltpu.VMEM((n, 2) + block, bf16),
            pltpu.VMEM((n, 4, 2) + block, bf16),
            pltpu.VMEM((n, 2, 4) + block, bf16),
            pltpu.VMEM((n, 2, 2) + block, bf16),
            pltpu.VMEM((n, 2) + block, bf16),
            pltpu.VMEM((n, 2) + block, bf16),
            pltpu.VMEM((n, 2) + block, bf16),
            pltpu.VMEM((n, 2) + block, bf16),
            pltpu.VMEM((tok_rows, width), jnp.float32),
            pltpu.VMEM((2, tok_rows, most), jnp.int32),
            pltpu.VMEM((2, tok_rows, most), jnp.int32),
            pltpu.VMEM((4, n, 1, lanes), jnp.int32),
            dma((n,)), dma((n,)),
            dma((n, 2)), dma((n, 2)),
            dma((n, 2)), dma((n, 2)),
            dma((n, 2)), dma((n, 2)),
            dma((n, 2)), dma((n, 2)),
            dma((n,)), dma((n,)),
            dma((n,)), dma((n,)),
            dma((3,)), dma((3,)),
            dma((4,)),
        ],
        compiler_params=pltpu.CompilerParams(
            collective_id=0, has_side_effects=True, vmem_limit_bytes=60 * 1024 * 1024
        ),
    )(
        tokens, expert_ids, expert_ids.T, gate_units,
        jnp.pad(capacity, (0, lanes - n))[None, :], w_gate, w_up, w_down,
    )


def solution(mesh):
    return jax.shard_map(
        local,
        mesh=mesh,
        in_specs=(
            P(("dp", "expert"), None),
            P(("dp", "expert"), None),
            P(("dp", "expert"), None),
            P(),
            P("expert", None, "dp"),
            P("expert", None, "dp"),
            P("expert", None, "dp"),
        ),
        out_specs=P(("dp", "expert"), None),
        check_vma=False,
    )
```

```python
import functools

import jax
import jax.numpy as jnp
from jax import lax
from jax.experimental import pallas as pl
from jax.experimental.pallas import tpu as pltpu
from jax.sharding import PartitionSpec as P

MESH = pl.DeviceIdType.MESH


def exchange(
    n, most, tok_ref, turned_ref, units_ref, cap_ref, wg_hbm, wu_hbm, wd_hbm, out_ref,
    wgu_ref, wd_ref, outgoing, xin, part, got1, sums, got2, ans, back, acc, code, scale, table,
    zs, zr, as_, ar, bs, br, cs, cr, ds, dr, es, er, ks, kr, ts, tr, loc,
):
    d = lax.axis_index("dp")
    e = lax.axis_index("expert")
    across = d + 1 - 2 * lax.rem(d, 2)
    along = lax.rem(d + 2, 4)
    diagonal = lax.rem(across + 2, 4)
    half = xin.shape[4]
    tok_rows = tok_ref.shape[0]
    lanes = table.shape[3]
    hidden_units = wd_ref.shape[0]
    near = ((across, e), (along, e))
    f32, bf16 = jnp.float32, jnp.bfloat16

    def remote(src, dst, send, recv, device):
        return pltpu.make_async_remote_copy(
            src_ref=src, dst_ref=dst, send_sem=send, recv_sem=recv,
            device_id=device, device_id_type=MESH,
        )

    def ahead(k):
        return (d, lax.rem(e + k, n))

    def behind(k):
        return (d, lax.rem(e + n - k, n))

    def to_owner(k):
        return remote(outgoing.at[k], xin.at[k, 0], zs.at[k], zr.at[k], ahead(k))

    def spread(i, r):
        return remote(xin.at[i, 0], xin.at[i, 1 + r], as_.at[i, r], ar.at[i, r], near[r])

    def relay(i, r):
        return remote(
            xin.at[i, 1 + r, r], xin.at[i, 3, r], bs.at[i, r], br.at[i, r], near[1 - r]
        )

    def first(i, r):
        return remote(
            part.at[i, r, pl.ds(0, 2)], got1.at[i, r], cs.at[i, r], cr.at[i, r], near[r]
        )

    def second(i, r):
        return remote(sums.at[i, r], got2.at[i, r], ds.at[i, r], dr.at[i, r], near[1 - r])

    def give_back(i):
        return remote(ans.at[i], back.at[i], es.at[i], er.at[i], behind(i))

    def count_out(k):
        return remote(table.at[0, 0], table.at[0, k], ks.at[k], kr.at[k], ahead(k))

    def table_near(r):
        return remote(table.at[0], table.at[1 + r], ts.at[r], tr.at[r], near[r])

    def table_far():
        return remote(table.at[1], table.at[3], ts.at[2], tr.at[2], near[1])

    def weights():
        pairs = (
            (wg_hbm, wgu_ref.at[pl.ds(0, hidden_units)]),
            (wu_hbm, wgu_ref.at[pl.ds(hidden_units, hidden_units)]),
            (wd_hbm, wd_ref),
        )
        return [
            pltpu.make_async_copy(hbm, vmem, loc.at[1 + w]) for w, (hbm, vmem) in enumerate(pairs)
        ]

    barrier = pltpu.get_barrier_semaphore()

    def greet(k, carry):
        pl.semaphore_signal(barrier, inc=1, device_id=ahead(k), device_id_type=MESH)
        return carry

    lax.fori_loop(1, n, greet, 0)
    for r in range(2):
        pl.semaphore_signal(barrier, inc=1, device_id=near[r], device_id_type=MESH)
    for copy in weights():
        copy.start()

    def iota(shape, axis):
        return lax.broadcasted_iota(jnp.int32, shape, axis)

    square = (tok_rows, tok_rows)
    turned = turned_ref[...]

    def upright(row):
        return jnp.broadcast_to(row, square).T[:, :1]

    ids = [upright(turned[k:k + 1, :]) for k in range(2)]
    hot = [(iota((tok_rows, lanes), 1) == ids[k]) for k in range(2)]
    named = jnp.where(hot[0] | hot[1], 1.0, 0.0)
    table[0, 0] = jnp.sum(named, axis=0, keepdims=True).astype(jnp.int32)
    lower = jnp.where(iota(square, 1) < iota(square, 0), 1.0, 0.0).astype(bf16)
    before = jnp.dot(lower, named.astype(bf16), preferred_element_type=f32)
    rank = [jnp.sum(jnp.where(h, before, 0.0), axis=1, keepdims=True) for h in hot]
    for k in range(2):
        slot = ids[k] * most + rank[k].astype(jnp.int32)
        code[k] = jnp.broadcast_to(slot, (tok_rows, most))

    hot_t = [(iota((n, tok_rows), 0) == turned[k:k + 1, :]) for k in range(2)]
    named_t = jnp.where(hot_t[0] | hot_t[1], 1.0, 0.0).astype(bf16)
    upper = jnp.where(iota(square, 0) < iota(square, 1), 1.0, 0.0).astype(bf16)
    before_t = jnp.dot(named_t, upper, preferred_element_type=f32)
    code_t = [
        turned[k:k + 1, :] * most
        + jnp.sum(jnp.where(hot_t[k], before_t, 0.0), axis=0, keepdims=True).astype(jnp.int32)
        for k in range(2)
    ]

    def rows_for(p, h):
        wanted = iota((most, tok_rows), 0) + p * most
        placing = jnp.where((code_t[0] == wanted) | (code_t[1] == wanted), 1.0, 0.0).astype(bf16)
        return jnp.dot(
            placing, tok_ref[:, h * half:(h + 1) * half], preferred_element_type=f32
        ).astype(bf16)

    for h in range(2):
        xin[0, 0, h] = rows_for(e, h)

    pl.semaphore_wait(barrier, n + 1)

    def counted(k, carry):
        count_out(k).start()
        return carry

    def launch(k, carry):
        for h in range(2):
            outgoing[k, h] = rows_for(ahead(k)[1], h)
        to_owner(k).start()
        return carry

    for r in range(2):
        spread(0, r).start()
    lax.fori_loop(1, n, counted, 0)
    lax.fori_loop(1, n, launch, 0)
    acc[...] = jnp.zeros_like(acc)

    def stage_a(i):
        @pl.when(i > 0)
        def _():
            to_owner(i).wait_recv()
            for r in range(2):
                spread(i, r).start()

    def stage_b(i):
        for r in range(2):
            spread(i, r).wait_recv()
            relay(i, r).start()

    def stage_c(i):
        @pl.when(i == 0)
        def _():
            for copy in weights():
                copy.wait()

        for r in range(2):
            relay(i, r).wait_recv()
        both = None
        for h in range(2):
            rows = xin[i, :, h].reshape(4 * most, half)
            term = lax.dot_general(
                rows, wgu_ref[:, h * half:(h + 1) * half], (((1,), (1,)), ((), ())),
                preferred_element_type=f32,
            )
            both = term if h == 0 else both + term
        gate, up = both[:, :hidden_units], both[:, hidden_units:]
        hidden = (gate / (1.0 + jnp.exp(-gate)) * up).astype(bf16)
        for h in range(2):
            made = jnp.dot(
                hidden, wd_ref[:, h * half:(h + 1) * half], preferred_element_type=f32
            )
            for slot, block in enumerate(((1, 3, 0, 2), (2, 3, 0, 1))[h]):
                part[i, h, slot] = made[block * most:(block + 1) * most].astype(bf16)
            first(i, h).start()

    def stage_d(i):
        for r in range(2):
            first(i, r).wait_recv()
            total = part[i, r, 3].astype(f32) + got1[i, r, 1].astype(f32)
            sums[i, r] = total.astype(bf16)
            second(i, r).start()

    def stage_e(i):
        for r in range(2):
            second(i, r).wait_recv()
            total = (
                part[i, r, 2].astype(f32) + got1[i, r, 0].astype(f32) + got2[i, r].astype(f32)
            )
            ans[i, r] = total.astype(bf16)

        @pl.when(i > 0)
        def _():
            give_back(i).start()

        @pl.when(i == 0)
        def _():
            kept_here = pltpu.make_async_copy(ans.at[0], back.at[0], loc.at[0])
            kept_here.start()
            kept_here.wait()

    def stage_f(i):
        @pl.when(i > 0)
        def _():
            give_back(i).wait_recv()

        wanted = iota((tok_rows, most), 1) + ahead(i)[1] * most
        placed = jnp.where(code[0] == wanted, scale[0], 0) + jnp.where(code[1] == wanted, scale[1], 0)
        low = placed & 7
        high = (placed - low).astype(f32).astype(bf16)
        low = low.astype(f32).astype(bf16)
        for h in range(2):
            rows = back[i, h]
            acc[:, h * half:(h + 1) * half] += jnp.dot(
                high, rows, preferred_element_type=f32
            ) + jnp.dot(low, rows, preferred_element_type=f32)

    def counts_near():
        def arrived(k, carry):
            count_out(k).wait_recv()
            return carry

        lax.fori_loop(1, n, arrived, 0)
        for r in range(2):
            table_near(r).start()

    def counts_far():
        for r in range(2):
            table_near(r).wait_recv()
        table_far().start()

    def counts_used():
        table_far().wait_recv()
        here = d * n + e
        offsets = jnp.zeros((1, lanes), jnp.int32)
        for s, row in enumerate((d, across, along, diagonal)):
            def add(k, total, s=s, row=row):
                earlier = row * n + behind(k)[1] < here
                return total + table[s, k] * earlier.astype(jnp.int32)

            offsets = lax.fori_loop(0, n, add, offsets)
        most_taken = lax.fori_loop(
            0, n,
            lambda j, row: jnp.where(iota((1, lanes), 1) == j, cap_ref[j], row),
            jnp.zeros((1, lanes), jnp.int32),
        )
        room = (most_taken - offsets).astype(f32)
        for k in range(2):
            limit = jnp.sum(jnp.where(hot[k], room, 0.0), axis=1, keepdims=True)
            units = jnp.where(rank[k] < limit, upright(units_ref[k:k + 1, :]), 0)
            scale[k] = jnp.broadcast_to(units, (tok_rows, most))

    stages = ((0, stage_a), (2, stage_b), (6, stage_d), (8, stage_e), (4, stage_c), (10, stage_f))

    def step(t, carry):
        for lag, stage in stages:
            @pl.when((t >= lag) & (t < n + lag))
            def _(stage=stage, lag=lag):
                stage(t - lag)
        for when, chore in ((3, counts_near), (5, counts_far), (7, counts_used)):
            pl.when(t == when)(chore)
        return carry

    lax.fori_loop(0, n + stages[-1][0], step, 0)
    out_ref[...] = (acc[...] * (1.0 / 1024.0)).astype(out_ref.dtype)

    def settle(i, carry):
        for r in range(2):
            spread(i, r).wait_send()
            relay(i, r).wait_send()
            first(i, r).wait_send()
            second(i, r).wait_send()

        @pl.when(i > 0)
        def _():
            to_owner(i).wait_send()
            give_back(i).wait_send()
            count_out(i).wait_send()

        return carry

    lax.fori_loop(0, n, settle, 0)
    for r in range(2):
        table_near(r).wait_send()
    table_far().wait_send()


def local(tokens, expert_ids, gate_units, capacity, w_gate, w_up, w_down):
    tok_rows, width = tokens.shape
    n = capacity.shape[0]
    most = max(2, 5 * tok_rows // (2 * n))
    most = -(-most // 8) * 8
    half = width // 2
    lanes = -(-n // 128) * 128
    bf16 = jnp.bfloat16
    vmem = pl.BlockSpec(memory_space=pltpu.VMEM)
    hbm = pl.BlockSpec(memory_space=pl.ANY)
    dma = pltpu.SemaphoreType.DMA
    block = (most, half)
    return pl.pallas_call(
        functools.partial(exchange, n, most),
        out_shape=jax.ShapeDtypeStruct(tokens.shape, bf16),
        in_specs=[vmem] * 3 + [pl.BlockSpec(memory_space=pltpu.SMEM)] + [hbm] * 3,
        out_specs=vmem,
        scratch_shapes=[
            pltpu.VMEM((2 * w_gate.shape[2], width), bf16),
            pltpu.VMEM((w_down.shape[2], width), bf16),
            pltpu.VMEM((n, 2) + block, bf16),
            pltpu.VMEM((n, 4, 2) + block, bf16),
            pltpu.VMEM((n, 2, 4) + block, bf16),
            pltpu.VMEM((n, 2, 2) + block, bf16),
            pltpu.VMEM((n, 2) + block, bf16),
            pltpu.VMEM((n, 2) + block, bf16),
            pltpu.VMEM((n, 2) + block, bf16),
            pltpu.VMEM((n, 2) + block, bf16),
            pltpu.VMEM((tok_rows, width), jnp.float32),
            pltpu.VMEM((2, tok_rows, most), jnp.int32),
            pltpu.VMEM((2, tok_rows, most), jnp.int32),
            pltpu.VMEM((4, n, 1, lanes), jnp.int32),
            dma((n,)), dma((n,)),
            dma((n, 2)), dma((n, 2)),
            dma((n, 2)), dma((n, 2)),
            dma((n, 2)), dma((n, 2)),
            dma((n, 2)), dma((n, 2)),
            dma((n,)), dma((n,)),
            dma((n,)), dma((n,)),
            dma((3,)), dma((3,)),
            dma((4,)),
        ],
        compiler_params=pltpu.CompilerParams(
            collective_id=0, has_side_effects=True, vmem_limit_bytes=60 * 1024 * 1024
        ),
    )(
        tokens, expert_ids.T, gate_units.T, capacity, w_gate[0].T, w_up[0].T, w_down[0].T,
    )


def solution(mesh):
    return jax.shard_map(
        local,
        mesh=mesh,
        in_specs=(
            P(("dp", "expert"), None),
            P(("dp", "expert"), None),
            P(("dp", "expert"), None),
            P(),
            P("expert", None, "dp"),
            P("expert", None, "dp"),
            P("expert", None, "dp"),
        ),
        out_specs=P(("dp", "expert"), None),
        check_vma=False,
    )
```
